512 devices in a mesh: dp: 64 (over x, z_lo, y), tensor: 8 (over z_hi, core).
Axes of the slice: x: 4, y: 8, z: 8 (z_hi: 4, z_lo: 2; z = z_hi * 2 + z_lo), core: 2. Of those that a mesh axis runs over, the one named last changes fastest.
Arguments:
- layer_input: bfloat16 [2560, 5120], P('dp', 'tensor'), may hold values from -6 to 6
- up_weight: bfloat16 [5120, 13824], P('dp', 'tensor'), may hold values from -0.078125 to 0.078125
- grad_output: bfloat16 [2560, 13824], P('dp', 'tensor'), may hold values from -60 to 60
- factor_input: float32 [5120, 5120], P('dp', 'tensor'), may hold values from -4 to 15, as said below
- factor_grad: float32 [13824, 13824], P('dp', 'tensor'), may hold values from -4 to 15, as said below
- decay: float32 [1], replicated, may hold values from 0.5 to 0.95
Outputs:
- grad_weight: float32 [5120, 13824], P('dp', 'tensor')
- grad_input: bfloat16 [2560, 5120], P('tensor', 'dp')
- new_factor_input: float32 [5120, 5120], P('dp', 'tensor')
- new_factor_grad: float32 [13824, 13824], P('dp', 'tensor')
The draws below stay inside these ranges and needn't reach their ends.
Inputs may be any that keep to these rules, and one draw needn't show every extreme that they name: `factor_input`: symmetric. `factor_grad`: symmetric.
All inputs are finite; a program needn't handle non-finite values.
Results may differ from the reference program's by a relative error of at most 0.001.
Values may be sent and summed in bfloat16 or wider, within the bound.
No kernel may reach another device: no remote copies, remote signals or barrier semaphores. Data moves between devices by JAX's collectives and lax.ppermute only.
A program may use at most 128 MiB of HBM per device.

```python
import math
import jax
import jax.numpy as jnp
from jax import lax

D = 5120
FF = 13824
TOKENS = 2560


def draw_grad_output(key, part):
    first = jax.random.fold_in(key, 11)
    second = jax.random.fold_in(key, 12)
    third = jax.random.fold_in(key, 13)
    row_scale = jnp.exp(jax.random.uniform(second, (TOKENS, 1), jnp.float32, math.log(0.3), math.log(3.0)))
    col_scale = jnp.exp(jax.random.uniform(third, (1, FF), jnp.float32, math.log(0.3), math.log(3.0)))
    base = jnp.clip(jax.random.normal(first, (TOKENS, FF), jnp.float32), -6.0, 6.0)
    return (base * row_scale * col_scale).astype(jnp.bfloat16)


def symmetric_factor(key, order):
    first = jax.random.fold_in(key, 21)
    second = jax.random.fold_in(key, 22)
    loose = jnp.clip(jax.random.normal(first, (order, order), jnp.float32), -4.0, 4.0) * 0.3
    middle = 0.5 * (loose + loose.T)
    lead = jnp.exp(jax.random.uniform(second, (order,), jnp.float32, 0.0, math.log(10.0)))
    return middle + jnp.diag(lead)


def draw_factor_input(key, part):
    return symmetric_factor(jax.random.fold_in(key, 31), D)


def draw_factor_grad(key, part):
    return symmetric_factor(jax.random.fold_in(key, 32), FF)


def level_of(own_key, dims, cuts, smallest, top_value):
    factor_of, own = 1.0, jax.random.fold_in(own_key, 6)
    for position, shards_of in cuts:
        draws = jnp.exp(jax.random.uniform(jax.random.fold_in(own, position), (shards_of,), jnp.float32, smallest / len(cuts), top_value / len(cuts)))
        factor_of = factor_of * jnp.repeat(draws, dims[position] // shards_of).reshape([-1 if axis == position else 1 for axis in range(len(dims))])
    return factor_of


def noise(stream_key, extent, width, limit, cuts=(), kind=jnp.bfloat16):
    gain = level_of(stream_key, extent, cuts, -0.22, 0.18) if cuts else 1.0
    result = jax.random.normal(stream_key, extent, jnp.float32) * width * gain
    return jnp.minimum(jnp.maximum(result, -limit), limit).astype(kind)


def setup_inputs(seed: int = 0) -> dict:
    splits = jax.random.split(jax.random.key(seed), 7)
    layer_input = noise(splits[0], (TOKENS, D), 1.0, 6.0, ((0, 64), (1, 8)))
    up_weight = noise(splits[1], (D, FF), D ** -0.5, 0.078125, ((0, 64), (1, 8)))
    grad_output = draw_grad_output(jax.random.fold_in(splits[6], 71), 0)
    factor_input = draw_factor_input(jax.random.fold_in(splits[6], 71), 0)
    factor_grad = draw_factor_grad(jax.random.fold_in(splits[6], 71), 0)
    decay = jnp.clip(jax.random.uniform(splits[5], (1,), jnp.float32, 0.5, 0.95), 0.5, 0.95)
    return dict(layer_input=layer_input, up_weight=up_weight, grad_output=grad_output, factor_input=factor_input, factor_grad=factor_grad, decay=decay)


def contract_rows(left, right):
    return lax.dot_general(left.astype(jnp.float32), right.astype(jnp.float32), (((0,), (0,)), ((), ())), preferred_element_type=jnp.float32)


def reference(layer_input, up_weight, grad_output, factor_input, factor_grad, decay):
    keep = decay[0]
    blend = (1.0 - keep) / TOKENS
    grad_weight = contract_rows(layer_input, grad_output)
    grad_input = lax.dot_general(grad_output.astype(jnp.float32), up_weight.astype(jnp.float32), (((1,), (1,)), ((), ())), preferred_element_type=jnp.float32).astype(jnp.bfloat16)
    new_factor_input = keep * factor_input + blend * contract_rows(layer_input, layer_input)
    new_factor_grad = keep * factor_grad + blend * contract_rows(grad_output, grad_output)
    return grad_weight, grad_input, new_factor_input, new_factor_grad
```

```python
import jax
import jax.numpy as jnp
from jax import lax
from jax.experimental import pallas as pl
from jax.experimental.pallas import tpu as pltpu
from jax.experimental.layout import Layout, with_layout_constraint
from jax.sharding import Mesh
from jax.sharding import PartitionSpec as P


AXES = ("dp_0", "dp_1", "dp_2", "tensor_0", "tensor_1")
DP = AXES[:3]
TENSOR = AXES[3:]
SIZES = (4, 2, 8, 4, 2)
X, ZL, Y, ZH, C = range(5)


def number(at):
    total = 0
    for place, size in zip(at, SIZES, strict=True):
        total = total * size + place % size
    return total


def pairs_of(move):
    out = []
    for i in range(512):
        at, rest = [], i
        for size in reversed(SIZES):
            at.append(rest % size)
            rest //= size
        at = at[::-1]
        out.append((i, number(move(list(at)))))
    return out


def towards(dim, turn):
    def move(at):
        step = 1 if (at[dim] + at[C]) % 2 == 0 else -1
        at[dim] += step if turn == 0 else -step
        return at

    return pairs_of(move)


def flipped(dim):
    def move(at):
        at[dim] = 1 - at[dim]
        return at

    return pairs_of(move)


def shifted(dim, by):
    def move(at):
        at[dim] += by
        return at

    return pairs_of(move)


Y_A, Y_B = towards(Y, 0), towards(Y, 1)
X_A, X_B = towards(X, 0), towards(X, 1)
H_A, H_B = towards(ZH, 0), towards(ZH, 1)
ZL_SWAP, C_SWAP = flipped(ZL), flipped(C)
TURN = pairs_of(lambda at: [at[ZH], at[C], at[Y], at[X], at[ZL]])


def rows_major(x):
    return with_layout_constraint(x, Layout(major_to_minor=tuple(range(x.ndim))))


def send(x, pairs):
    return rows_major(lax.ppermute(rows_major(x), AXES, pairs))


def contract_rows(left, right):
    return lax.dot_general(
        left, right, (((0,), (0,)), ((), ())), preferred_element_type=jnp.float32
    )


def contract_cols(left, right):
    return lax.dot_general(
        left, right, (((1,), (1,)), ((), ())), preferred_element_type=jnp.float32
    )


def copy_block(_, source, target):
    target[...] = source[...]


def picked_blocks(x, order):
    block = (1, *x.shape[1:])
    return pl.pallas_call(
        copy_block,
        grid_spec=pltpu.PrefetchScalarGridSpec(
            num_scalar_prefetch=1,
            grid=(x.shape[0],),
            in_specs=[pl.BlockSpec(block, lambda i, at: (at[i], 0, 0))],
            out_specs=pl.BlockSpec(block, lambda i, at: (i, 0, 0)),
        ),
        out_shape=jax.ShapeDtypeStruct(x.shape, x.dtype),
        name="picked_blocks",
    )(order, x)


def sign(n):
    return 1 - 2 * (n % 2)


def local(layer_input, up_weight, grad_output, factor_input, factor_grad, decay):
    tokens = layer_input.shape[0]
    feats, units = up_weight.shape[0], factor_grad.shape[0]
    wide_x, wide_g = layer_input.shape[1], grad_output.shape[1]
    token_total = tokens * 64
    keep = decay[0]
    blend = (1.0 - keep) / token_total
    x, zl, y, zh, c = (lax.axis_index(a) for a in AXES)
    own_core = c == zl
    dx, dy = sign(x + c), sign(y + c)

    p0 = jnp.concatenate([layer_input, grad_output], axis=1)
    q_own = send(grad_output, ZL_SWAP)

    def along_y(own):
        a1 = send(own, Y_A)
        a2 = send(jnp.concatenate([own, a1], 0), Y_B)
        a3 = send(a2, Y_A)
        a4 = send(a3, Y_B)
        return a1, a2, a3, a4

    n = tokens
    a1, a2, a3, a4 = along_y(p0)
    by_y = jnp.zeros((8, n, wide_x + wide_g), p0.dtype)
    for piece, k in (
        (p0, 0), (a1, 1), (a2[:n], -1), (a2[n:], -2),
        (a3[:n], 2), (a3[n:], 3), (a4[:n], -3), (a4[n:], -4),
    ):
        by_y = lax.dynamic_update_index_in_dim(by_y, piece, (y + dy * k) % 8, 0)
    rows = 8 * n
    by_y = by_y.reshape(rows, wide_x + wide_g)
    p1 = send(by_y, X_A)
    p2 = send(by_y, X_B)
    p3 = send(p1, X_B)
    p_wide = (by_y, p1, p2, p3)

    b1 = send(q_own, X_A)
    b2 = send(jnp.concatenate([q_own, b1], 0), X_B)
    by_x = jnp.zeros((4, n, wide_g), q_own.dtype)
    for piece, k in ((q_own, 0), (b1, 1), (b2[:n], -1), (b2[n:], -2)):
        by_x = lax.dynamic_update_index_in_dim(by_x, piece, (x + dx * k) % 4, 0)
    by_x = by_x.reshape(4 * n, wide_g)
    q_wide = (by_x, *along_y(by_x))

    part = jnp.concatenate(
        [
            lax.dynamic_slice_in_dim(by_y, y * feats, feats, 1),
            lax.dynamic_slice_in_dim(by_y, wide_x + y * units, units, 1),
        ],
        axis=1,
    )
    narrow = feats + units
    h0 = send(part, TURN)
    h1 = send(h0, H_A)
    h2 = send(jnp.concatenate([h0, h1], 0), H_B)
    mine = jnp.concatenate([h0, h1, h2], 0)
    theirs = send(mine, C_SWAP)
    n_own = jnp.where(own_core, mine, theirs)
    n_other = jnp.where(own_core, theirs, mine)
    n_cross = send(n_other[:, :feats], ZL_SWAP)

    def place(x_at, step):
        off = (x_at - zh) * step % 4
        return off ^ (off >> 1)

    order_k = jnp.array([0, 1, -1, -2], jnp.int32)
    order_p = place((x + dx * order_k) % 4, sign(zh + zl))
    l_own = picked_blocks(
        jnp.concatenate([n_own, n_cross], 1).reshape(4, rows, narrow + feats), order_p
    ).reshape(4 * rows, narrow + feats)
    order_y = (y + dy * jnp.array([0, 1, -1, -2, 2, 3, -3, -4], jnp.int32)) % 8
    x_at = jnp.arange(4, dtype=jnp.int32)
    order_q = place(x_at[None, :], sign(zh + 1 - zl)) * 8 + order_y[:, None]
    l_other = picked_blocks(n_other.reshape(32, n, narrow), order_q.reshape(32)).reshape(
        4 * rows, narrow
    )

    total = None
    fi_total = None
    gi_p, gi_q = [], []
    at = 0
    for piece in q_wide:
        got = contract_rows(l_other[at : at + piece.shape[0]], piece)
        total = got if total is None else total + got
        gi_q.append(contract_cols(piece, up_weight))
        at += piece.shape[0]
    at = 0
    for piece in p_wide:
        left = l_own[at : at + piece.shape[0]]
        right_x, right_g = piece[:, :wide_x], piece[:, wide_x:]
        total = total + contract_rows(left[:, :narrow], right_g)
        got = contract_rows(
            jnp.concatenate([left[:, :feats], left[:, narrow:]], 1), right_x
        )
        fi_total = got if fi_total is None else fi_total + got
        gi_p.append(contract_cols(right_g, up_weight))
        at += piece.shape[0]
    grad_weight = total[:feats]
    new_factor_grad = keep * factor_grad + blend * total[feats:]
    fi_got = send(fi_total[feats:], ZL_SWAP)
    new_factor_input = keep * factor_input + blend * (fi_total[:feats] + fi_got)

    gi_p = jnp.concatenate(gi_p, 0).reshape(4, rows, feats)
    back = (x_at - x) * dx % 4
    gi_p = picked_blocks(gi_p, back ^ (back >> 1)).reshape(4, rows, feats)
    gi_q = jnp.concatenate(gi_q, 0).reshape(32, n, feats)
    back_y = (jnp.arange(8, dtype=jnp.int32) - y) * dy % 8
    spot = jnp.where(
        back_y < 2, back_y, jnp.where(back_y < 4, back_y + 2, jnp.where(back_y < 6, 11 - back_y, 9 - back_y))
    )
    gi_q = picked_blocks(gi_q, (spot[None, :] * 4 + x_at[:, None]).reshape(32)).reshape(
        4, rows, feats
    )
    gi_keep = jnp.where(own_core, gi_p, gi_q)
    gi_send = jnp.where(own_core, gi_q, gi_p)
    half = gi_keep + send(gi_send, C_SWAP)
    out = lax.dynamic_index_in_dim(half, zh, 0, keepdims=False)
    for by in (1, 3, 2):
        piece = lax.dynamic_index_in_dim(half, (zh + by) % 4, 0, keepdims=False)
        out = out + send(piece, shifted(ZH, by))
    return (grad_weight, out.astype(jnp.bfloat16), new_factor_input, new_factor_grad)


def solution(mesh):
    finer = Mesh(mesh.devices.reshape(SIZES), AXES)

    return jax.shard_map(
        local,
        mesh=finer,
        in_specs=(P(DP, TENSOR), P(DP, TENSOR), P(DP, TENSOR), P(DP, TENSOR), P(DP, TENSOR), P()),
        out_specs=(P(DP, TENSOR), P(TENSOR, DP), P(DP, TENSOR), P(DP, TENSOR)),
        check_vma=False,
    )
```

```python
import jax
import jax.numpy as jnp
from jax import lax
from jax.experimental.layout import Layout, with_layout_constraint
from jax.sharding import Mesh
from jax.sharding import PartitionSpec as P


AXES = ("dp_0", "dp_1", "dp_2", "tensor_0", "tensor_1")
DP = AXES[:3]
TENSOR = AXES[3:]
SIZES = (4, 2, 8, 4, 2)
X, ZL, Y, ZH, C = range(5)


def number(at):
    total = 0
    for place, size in zip(at, SIZES, strict=True):
        total = total * size + place % size
    return total


def pairs_of(move):
    out = []
    for i in range(512):
        at, rest = [], i
        for size in reversed(SIZES):
            at.append(rest % size)
            rest //= size
        at = at[::-1]
        out.append((i, number(move(list(at)))))
    return out


def towards(dim, turn):
    def move(at):
        step = 1 if (at[dim] + at[C]) % 2 == 0 else -1
        at[dim] += step if turn == 0 else -step
        return at

    return pairs_of(move)


def flipped(dim):
    def move(at):
        at[dim] = 1 - at[dim]
        return at

    return pairs_of(move)


Y_A, Y_B = towards(Y, 0), towards(Y, 1)
X_A, X_B = towards(X, 0), towards(X, 1)
H_A, H_B = towards(ZH, 0), towards(ZH, 1)
ZL_SWAP, C_SWAP = flipped(ZL), flipped(C)
TURN = pairs_of(lambda at: [at[ZH], at[C], at[Y], at[X], at[ZL]])


def rows_major(x):
    return with_layout_constraint(x, Layout(major_to_minor=tuple(range(x.ndim))))


def send(x, pairs):
    return rows_major(lax.ppermute(rows_major(x), AXES, pairs))


def contract_rows(left, right):
    return rows_major(
        lax.dot_general(
            left, right, (((0,), (0,)), ((), ())), preferred_element_type=jnp.float32
        )
    )


def contract_cols(left, right):
    return lax.dot_general(
        left, right, (((1,), (1,)), ((), ())), preferred_element_type=jnp.float32
    )


def placed(blocks, spots, count):
    whole = jnp.zeros((count, *blocks[0].shape), blocks[0].dtype)
    for block, spot in zip(blocks, spots, strict=True):
        whole = lax.dynamic_update_index_in_dim(whole, block, spot, 0)
    return whole


def row_of(x, at):
    return lax.dynamic_index_in_dim(x, at, 0, keepdims=False)


def sign(n):
    return 1 - 2 * (n % 2)


def local(layer_input, up_weight, grad_output, factor_input, factor_grad, decay):
    n = layer_input.shape[0]
    feats, units = up_weight.shape[0], factor_grad.shape[0]
    wide_x, wide_g = layer_input.shape[1], grad_output.shape[1]
    keep = decay[0]
    blend = (1.0 - keep) / (n * 64)
    x, zl, y, zh, c = (lax.axis_index(a) for a in AXES)
    own_core = c == zl
    dx, dy, dh = sign(x + c), sign(y + c), sign(zh + c)
    rows = 8 * n

    def along_y(own):
        a1 = send(own, Y_A)
        a2 = send(jnp.concatenate([own, a1], 0), Y_B)
        a3 = send(a2, Y_A)
        a4 = send(a3, Y_B)
        m = own.shape[0]
        blocks = (own, a1, a2[:m], a2[m:], a3[:m], a3[m:], a4[:m], a4[m:])
        return blocks, [(y + dy * k) % 8 for k in (0, 1, -1, -2, 2, 3, -3, -4)]

    def along_x(own):
        b1 = send(own, X_A)
        b2 = send(jnp.concatenate([own, b1], 0), X_B)
        m = own.shape[0]
        return placed((own, b1, b2[:m], b2[m:]), x_spots, 4)

    x_spots = [(x + dx * k) % 4 for k in (0, 1, -1, -2)]

    spare = jnp.zeros((n, -(wide_x + wide_g) % 128), grad_output.dtype)
    p0 = jnp.concatenate([layer_input, grad_output, spare], axis=1)
    by_y = placed(*along_y(p0), 8).reshape(rows, -1)
    p1 = send(by_y, X_A)
    p2 = send(by_y, X_B)
    p3 = send(p1, X_B)
    p_wide = (by_y, p1, p2, p3)

    by_x = along_x(send(grad_output, ZL_SWAP)).reshape(4 * n, wide_g)
    q_wide = placed(*along_y(by_x), 8).reshape(4 * rows, wide_g)

    w_pair = jnp.concatenate([up_weight, send(up_weight, ZL_SWAP)], 0)
    w_all = along_x(w_pair)
    w_own, w_other = (w.reshape(4 * feats, wide_g) for w in (w_all[:, :feats], w_all[:, feats:]))
    w_keep = jnp.where(own_core, w_own, w_other)
    w_send = jnp.where(own_core, w_other, w_own)

    part = jnp.concatenate(
        [
            lax.dynamic_slice_in_dim(by_y, y * feats, 128, 1),
            lax.dynamic_slice_in_dim(by_y, wide_x + y * units, 256, 1),
        ],
        axis=1,
    )
    h0 = send(part, TURN)
    h1 = send(h0, H_A)
    h2 = send(jnp.concatenate([h0, h1], 0), H_B)
    mine = placed(
        (h0, h1, h2[:rows], h2[rows:]), [(zh + dh * k) % 4 for k in (0, 1, -1, -2)], 4
    ).reshape(4 * rows, -1)
    theirs = send(mine, C_SWAP)
    n_own = jnp.where(own_core, mine, theirs)
    n_other = jnp.where(own_core, theirs, mine)
    n_cross = send(n_other[:, :128], ZL_SWAP)
    n_fi = jnp.concatenate([n_own[:, :128], n_cross], 1).reshape(4, rows, 256)
    n_own = n_own.reshape(4, rows, -1)

    mine_g = by_y[:, wide_x : wide_x + wide_g]
    half = contract_cols(w_keep, mine_g) + send(contract_cols(w_send, mine_g), C_SWAP)
    half = half.reshape(4, feats, rows)
    far = jnp.concatenate([row_of(half, (zh - dh) % 4), row_of(half, (zh - 2 * dh) % 4)], 0)
    far = send(far, H_B)
    near = row_of(half, (zh + dh) % 4) + far[feats:]
    grad_input = row_of(half, zh) + far[:feats] + send(near, H_A)
    grad_input = send(grad_input.astype(jnp.bfloat16), TURN).T

    n_other = n_other.reshape(4, 8, n, -1).transpose(1, 0, 2, 3).reshape(4 * rows, -1)
    total, fi_total = contract_rows(n_other, q_wide), 0.0
    for piece, spot in zip(p_wide, x_spots):
        total = total + contract_rows(row_of(n_own, spot), piece[:, wide_x : wide_x + wide_g])
        fi_total = fi_total + contract_rows(row_of(n_fi, spot), piece[:, :wide_x])
    grad_weight = total[:feats]
    new_factor_grad = keep * factor_grad + blend * total[128 : 128 + units]
    fi_got = send(fi_total[128 : 128 + feats], ZL_SWAP)
    new_factor_input = keep * factor_input + blend * (fi_total[:feats] + fi_got)
    return (grad_weight, grad_input, new_factor_input, new_factor_grad)


def solution(mesh):
    finer = Mesh(mesh.devices.reshape(SIZES), AXES)

    return jax.shard_map(
        local,
        mesh=finer,
        in_specs=(P(DP, TENSOR), P(DP, TENSOR), P(DP, TENSOR), P(DP, TENSOR), P(DP, TENSOR), P()),
        out_specs=(P(DP, TENSOR), P(TENSOR, DP), P(DP, TENSOR), P(DP, TENSOR)),
        check_vma=False,
    )
```

```python
import jax
import jax.numpy as jnp
from jax import lax
from jax.experimental.layout import Layout, with_layout_constraint
from jax.sharding import Mesh
from jax.sharding import PartitionSpec as P


AXES = ("dp_0", "dp_1", "dp_2", "tensor_0", "tensor_1")
DP = AXES[:3]
TENSOR = AXES[3:]
SIZES = (4, 2, 8, 4, 2)
X, ZL, Y, ZH, C = range(5)


def number(at):
    total = 0
    for place, size in zip(at, SIZES, strict=True):
        total = total * size + place % size
    return total


def pairs_of(move):
    out = []
    for i in range(512):
        at, rest = [], i
        for size in reversed(SIZES):
            at.append(rest % size)
            rest //= size
        at = at[::-1]
        out.append((i, number(move(list(at)))))
    return out


def towards(dim, turn):
    def move(at):
        step = 1 if (at[dim] + at[C]) % 2 == 0 else -1
        at[dim] += step if turn == 0 else -step
        return at

    return pairs_of(move)


def flipped(dim):
    def move(at):
        at[dim] = 1 - at[dim]
        return at

    return pairs_of(move)


Y_A, Y_B = towards(Y, 0), towards(Y, 1)
X_A, X_B = towards(X, 0), towards(X, 1)
H_A, H_B = towards(ZH, 0), towards(ZH, 1)
ZL_SWAP, C_SWAP = flipped(ZL), flipped(C)
CROSS = tuple(
    [p for p in pairs_of(move) if (p[0] // 64 + p[0]) % 2]
    for move in (
        lambda at: [at[X], 1 - at[ZL], at[Y], at[ZH], at[C]],
        lambda at: [at[X], 1 - at[ZL], at[Y], at[ZH], 1 - at[C]],
    )
)
TURN = pairs_of(lambda at: [at[ZH], at[C], at[Y], at[X], at[ZL]])
TURN_H_A = [(i, TURN[j][1]) for i, j in H_A]


def rows_major(x):
    return with_layout_constraint(x, Layout(major_to_minor=tuple(range(x.ndim))))


def send(x, pairs):
    return rows_major(lax.ppermute(rows_major(x), AXES, pairs))


def contract_rows(left, right):
    return rows_major(
        lax.dot_general(
            left, right, (((0,), (0,)), ((), ())), preferred_element_type=jnp.float32
        )
    )


def contract_cols(left, right):
    return lax.dot_general(
        left, right, (((1,), (1,)), ((), ())), preferred_element_type=jnp.float32
    )


def placed(blocks, spots, count):
    whole = jnp.zeros((count, *blocks[0].shape), blocks[0].dtype)
    for block, spot in zip(blocks, spots, strict=True):
        whole = lax.dynamic_update_index_in_dim(whole, block, spot, 0)
    return whole


def row_of(x, at):
    return lax.dynamic_index_in_dim(x, at, 0, keepdims=False)


def sign(n):
    return 1 - 2 * (n % 2)


def local(layer_input, up_weight, grad_output, factor_input, factor_grad, decay):
    n = layer_input.shape[0]
    feats, units = up_weight.shape[0], factor_grad.shape[0]
    wide_x, wide_g = layer_input.shape[1], grad_output.shape[1]
    keep = decay[0]
    blend = (1.0 - keep) / (n * 64)
    x, zl, y, zh, c = (lax.axis_index(a) for a in AXES)
    own_core = c == zl
    dx, dy, dh = sign(x + c), sign(y + c), sign(zh + c)
    rows = 8 * n

    def along_y(own):
        a1 = send(own, Y_A)
        a2 = send(jnp.concatenate([own, a1], 0), Y_B)
        a3 = send(a2, Y_A)
        a4 = send(a3, Y_B)
        m = own.shape[0]
        blocks = (own, a1, a2[:m], a2[m:], a3[:m], a3[m:], a4[:m], a4[m:])
        return blocks, [(y + dy * k) % 8 for k in (0, 1, -1, -2, 2, 3, -3, -4)]

    def along_x(own):
        b1 = send(own, X_A)
        pair = jnp.concatenate([own, b1], 0)
        b2 = send(pair, X_B)
        m = own.shape[0]
        return placed((own, b1, b2[:m], b2[m:]), x_spots, 4)

    x_spots = [(x + dx * k) % 4 for k in (0, 1, -1, -2)]

    spare = jnp.zeros((n, -(wide_x + wide_g) % 128), grad_output.dtype)
    p0 = jnp.concatenate([layer_input, grad_output, spare], axis=1)
    by_y = placed(*along_y(p0), 8).reshape(rows, -1)
    p1 = send(by_y, X_A)
    p2 = send(by_y, X_B)
    p3 = send(p1, X_B)
    p_wide = (by_y, p1, p2, p3)

    by_x = along_x(send(grad_output, ZL_SWAP)).reshape(4 * n, wide_g)
    q_wide = placed(*along_y(by_x), 8).reshape(4 * rows, wide_g)

    w_pair = jnp.concatenate([up_weight, send(up_weight, ZL_SWAP)], 0)
    w_all = along_x(w_pair)
    w_own, w_other = (w.reshape(4 * feats, wide_g) for w in (w_all[:, :feats], w_all[:, feats:]))
    w_keep = jnp.where(own_core, w_own, w_other)
    w_send = jnp.where(own_core, w_other, w_own)

    part = jnp.concatenate(
        [
            lax.dynamic_slice_in_dim(by_y, y * feats, 128, 1),
            lax.dynamic_slice_in_dim(by_y, wide_x + y * units, 256, 1),
        ],
        axis=1,
    )
    h0 = send(part, TURN)
    h1 = send(h0, H_A)

    mine_g = by_y[:, wide_x : wide_x + wide_g]
    half = contract_cols(w_keep, mine_g) + send(contract_cols(w_send, mine_g), C_SWAP)
    half = half.reshape(4, feats, rows)
    far = jnp.concatenate([row_of(half, (zh - dh) % 4), row_of(half, (zh - 2 * dh) % 4)], 0)
    high = lax.reduce_precision(far, 8, 7)
    far = jnp.concatenate([high, far - high], 0).astype(jnp.bfloat16)
    far = jnp.pad(far, ((0, 0), (0, h0.shape[1] - rows)))
    h2 = send(jnp.concatenate([h0, h1, far], 0), H_B)
    far = h2[2 * rows :, :rows].astype(jnp.float32)
    far = far[: 2 * feats] + far[2 * feats :]
    here = row_of(half, zh) + far[:feats]
    near = row_of(half, (zh + dh) % 4) + far[feats:]
    here, near = send(here, TURN), send(near, TURN_H_A)
    grad_input = (here + near).astype(jnp.bfloat16).T

    mine = placed(
        (h0, h1, h2[:rows], h2[rows : 2 * rows]),
        [(zh + dh * k) % 4 for k in (0, 1, -1, -2)],
        4,
    ).reshape(4 * rows, -1)
    theirs = send(mine, C_SWAP)
    n_own = jnp.where(own_core, mine, theirs)
    n_other = jnp.where(own_core, theirs, mine)
    n_cross = jnp.where(own_core, send(mine[:, :128], CROSS[0]), send(mine[:, :128], CROSS[1]))
    n_fi = jnp.concatenate([n_own[:, :128], n_cross], 1).reshape(4, rows, 256)
    n_own = n_own.reshape(4, rows, -1)

    n_other = n_other.reshape(4, 8, n, -1).transpose(1, 0, 2, 3).reshape(4 * rows, -1)
    fi_total = 0.0
    for piece, spot in zip(p_wide, x_spots):
        fi_total = fi_total + contract_rows(row_of(n_fi, spot), piece[:, :wide_x])
    total = contract_rows(n_other, q_wide)
    for piece, spot in zip(p_wide, x_spots):
        total = total + contract_rows(row_of(n_own, spot), piece[:, wide_x : wide_x + wide_g])
    grad_weight = total[:feats]
    new_factor_grad = keep * factor_grad + blend * total[128 : 128 + units]
    fi_got = send(fi_total[128 : 128 + feats], ZL_SWAP)
    new_factor_input = keep * factor_input + blend * (fi_total[:feats] + fi_got)
    return (grad_weight, grad_input, new_factor_input, new_factor_grad)


def solution(mesh):
    finer = Mesh(mesh.devices.reshape(SIZES), AXES)

    return jax.shard_map(
        local,
        mesh=finer,
        in_specs=(P(DP, TENSOR), P(DP, TENSOR), P(DP, TENSOR), P(DP, TENSOR), P(DP, TENSOR), P()),
        out_specs=(P(DP, TENSOR), P(TENSOR, DP), P(DP, TENSOR), P(DP, TENSOR)),
        check_vma=False,
    )
```
